32 devices in a mesh: dp: 8 (over z, x), mp: 4 (over y, core).
Axes of the slice: x: 2, y: 2, z: 4, core: 2. Of those that a mesh axis runs over, the one named last changes fastest.
Arguments:
- hidden_in: bfloat16 [8192, 2048], P('dp', 'mp'), may hold values from -6 to 6
- token_ids: int32 [8192], P('dp'), may hold values from 0 to 128001, as said below
- passage_counts: int32 [16], P('dp'), may hold values from 1 to 4, as said below
- positive_doc: int32 [1024], P('dp'), may hold values from 0 to 15
- queries: bfloat16 [1024, 2048], P('dp', 'mp'), may hold values from -6 to 6
- norm_gain: float32 [2048], replicated, may hold values from 0.5 to 1.5
- w_gate: bfloat16 [2048, 7168], P(None, 'mp'), may hold values from -0.125 to 0.125
- w_up: bfloat16 [2048, 7168], P(None, 'mp'), may hold values from -0.125 to 0.125
- w_down: bfloat16 [7168, 2048], P('mp'), may hold values from -0.0625 to 0.0625
Outputs:
- query_loss: float32 [1024], P('dp')
- hidden_grad: bfloat16 [8192, 2048], P('dp', 'mp')
The draws below stay inside these ranges and needn't reach their ends.
Inputs may be any that keep to these rules, and one draw needn't show every extreme that they name: `passage_counts`: A document has 1 to 4 passages; every draw has a dp index whose documents all have 4. The live passages hold 40 passages in all. `token_ids`: 128001 marks padding; it stands only at the tail of a document's last live passage, and every live passage has a token that is not padding.
All inputs are finite; a program needn't handle non-finite values.
Results may differ from the reference program's by a relative error of at most 0.023.
Values may be sent and summed in bfloat16 or wider, within the bound.
A program may use at most 128 MiB of HBM per device.

```python
import jax
import jax.numpy as jnp
from jax import lax

D = 2048
FF = 7168
L = 128
PMAX = 4
DOC_DEV = 2
CAP = 20
DOCS = 16
PASSAGES = 64
QUERIES = 1024
ROWS = 8192
N_DP = 8


pad_token = 128001


def make_counts(key):
    half = DOCS // 2
    order = jax.random.permutation(jax.random.fold_in(key, 101), half)
    base = 1 + order % PMAX
    heavy = jax.random.randint(jax.random.fold_in(key, 102), (), 0, half // DOC_DEV)
    base = jnp.where(jnp.arange(half) // DOC_DEV == heavy, PMAX, base)
    return jnp.concatenate([base, PMAX + 1 - base]).astype(jnp.int32)


def draw_passage_counts(key, part):
    return make_counts(key)


def draw_token_ids(key, part):
    counts = make_counts(key)
    passage_total = DOCS * PMAX
    passage_index = jnp.arange(passage_total, dtype=jnp.int32)
    last_live = passage_index % PMAX == jnp.repeat(counts, PMAX) - 1
    length = jax.random.randint(jax.random.fold_in(key, 106), (passage_total,), 1, L + 1)
    length = jnp.where(last_live, length, L)
    position = jnp.arange(L, dtype=jnp.int32)
    words = jax.random.randint(jax.random.fold_in(key, 107), (passage_total, L), 0, 128000)
    tokens = jnp.where(position[None, :] < length[:, None], words, pad_token)
    return tokens.reshape(passage_total * L).astype(jnp.int32)


def touch_ends(drawn, key, least, largest):
    place = [jax.random.randint(jax.random.fold_in(key, axis), (), 0, length) for axis, length in enumerate(drawn.shape)]
    widest = drawn.shape.index(max(drawn.shape))
    next_to = place[:widest] + [(place[widest] + 1) % drawn.shape[widest]] + place[widest + 1:]
    return drawn.at[tuple(place)].set(least).at[tuple(next_to)].set(largest)


def levels(own_key, extent, pieces, low, largest):
    def one(dim, shards_of):
        draws = jax.random.uniform(jax.random.fold_in(jax.random.fold_in(own_key, 6), dim), (shards_of,), jnp.float32, low / len(pieces), largest / len(pieces))
        return jnp.repeat(jnp.exp(draws), extent[dim] // shards_of).reshape((-1,) + (1,) * (len(extent) - dim - 1))

    level = one(*pieces[0])
    for cut in pieces[1:]:
        level = level * one(*cut)
    return level


def scatter_about(rng, dims, deviation, reach, cuts=(), kind=jnp.bfloat16):
    drawn = jax.random.normal(rng, dims, jnp.float32) * deviation
    if len(cuts) > 0:
        drawn = levels(rng, dims, cuts, -0.22, 0.18) * drawn
    return jnp.clip(drawn, min=-reach, max=reach).astype(kind)


def setup_inputs(seed: int = 0) -> dict:
    key_of = jax.random.split(jax.random.key(seed), 10)
    return {
        "hidden_in": scatter_about(key_of[0], (ROWS, D), 1.0, 6.0, ((0, 8), (1, 4))),
        "token_ids": draw_token_ids(jax.random.fold_in(key_of[9], 71), 0),
        "passage_counts": draw_passage_counts(jax.random.fold_in(key_of[9], 71), 0),
        "positive_doc": touch_ends(jax.random.randint(key_of[3], (QUERIES,), 0, DOCS), jax.random.fold_in(key_of[3], 1), 0, DOCS - 1).astype(jnp.int32),
        "queries": scatter_about(key_of[4], (QUERIES, D), 1.0, 6.0, ((0, 8), (1, 4))),
        "norm_gain": jnp.clip(1.0 + 0.1 * jax.random.normal(key_of[5], (D,), jnp.float32), 0.5, 1.5),
        "w_gate": scatter_about(key_of[6], (D, FF), D ** -0.5, 0.125, ((1, 4),)),
        "w_up": scatter_about(key_of[7], (D, FF), D ** -0.5, 0.125, ((1, 4),)),
        "w_down": scatter_about(key_of[8], (FF, D), FF ** -0.5, 0.0625, ((0, 4),)),
    }


pad_token = 128001
score_scale = 20.0
loss_seed = 4096.0
norm_epsilon = 1e-05
unit_epsilon = 1e-06

def layer_forward(rows, norm_gain, w_gate, w_up, w_down):
    row_float = rows.astype(jnp.float32)
    rms_scale = lax.rsqrt(lax.optimization_barrier(jnp.mean(row_float * row_float, axis=1, keepdims=True)) + norm_epsilon)
    normed = (row_float * rms_scale * norm_gain[None, :]).astype(jnp.bfloat16)
    gate = jnp.dot(normed, w_gate, preferred_element_type=jnp.float32)
    up = jnp.dot(normed, w_up, preferred_element_type=jnp.float32)
    sigmoid_gate = jax.nn.sigmoid(gate)
    hidden = (gate * sigmoid_gate * up).astype(jnp.bfloat16)
    branch = jnp.dot(hidden, w_down, preferred_element_type=jnp.float32)
    return (row_float, rms_scale, gate, up, sigmoid_gate, branch)

def reference(hidden_in, token_ids, passage_counts, positive_doc, queries, norm_gain, w_gate, w_up, w_down):
    block_len = L // 4
    block_total = DOCS * PMAX * 4
    block_index = jnp.arange(block_total, dtype=jnp.int32)
    live_block = block_index // 4 % PMAX < jnp.repeat(passage_counts, PMAX * 4)
    token_live = (token_ids.reshape(block_total, block_len) != pad_token) & live_block[:, None]
    chosen = jnp.nonzero(live_block, size=N_DP * CAP)[0].astype(jnp.int32)
    task_rows = hidden_in.reshape(block_total, block_len, D)[chosen].reshape(N_DP, CAP * block_len, D)
    task_row_mask = token_live[chosen].astype(jnp.float32).reshape(N_DP, CAP, block_len)

    def pool_group(pair):
        rows, mask = pair
        row_float, rms_scale, gate, up, sigmoid_gate, branch = layer_forward(rows, norm_gain, w_gate, w_up, w_down)
        output = (row_float + branch).reshape(CAP, block_len, D)
        return lax.optimization_barrier(jnp.sum(output * mask[:, :, None], axis=1))
    pooled = lax.map(pool_group, (task_rows, task_row_mask)).reshape(N_DP * CAP, D)
    block_sums = jnp.zeros((block_total, D), jnp.float32).at[chosen].set(pooled)
    passage_sum = block_sums.reshape(PASSAGES, 4, D).sum(axis=1)
    token_total = lax.optimization_barrier(jnp.sum(token_live.reshape(PASSAGES, L).astype(jnp.float32), axis=1))
    divisor = jnp.maximum(token_total, 1.0)
    passage_vec = (passage_sum / divisor[:, None]).astype(jnp.bfloat16)
    passage_live = live_block.reshape(PASSAGES, 4)[:, 0].astype(jnp.float32)
    vec_float = passage_vec.astype(jnp.float32)
    query_float = queries.astype(jnp.float32)
    raw_score = lax.dot_general(queries, passage_vec, (((1,), (1,)), ((), ())), preferred_element_type=jnp.float32)
    query_scale = lax.rsqrt(lax.optimization_barrier(jnp.sum(query_float * query_float, axis=1)) + unit_epsilon)
    passage_scale = lax.rsqrt(lax.optimization_barrier(jnp.sum(vec_float * vec_float, axis=1)) + unit_epsilon)
    scores = score_scale * raw_score * query_scale[:, None] * passage_scale[None, :]
    weights = passage_live[None, :] * jnp.exp(scores)
    doc_mass = weights.reshape(QUERIES, DOCS, PMAX).sum(axis=2)
    total_mass = doc_mass.sum(axis=1)
    positive_hit = (positive_doc[:, None] == jnp.arange(DOCS, dtype=jnp.int32)[None, :]).astype(jnp.float32)
    positive_mass = lax.optimization_barrier(jnp.sum(doc_mass * positive_hit, axis=1))
    query_loss = jnp.log(total_mass) - jnp.log(positive_mass)
    positive_pass = jnp.repeat(positive_hit, PMAX, axis=1)
    coefficient = loss_seed * score_scale * query_scale[:, None] * (weights / total_mass[:, None] - positive_pass * weights / positive_mass[:, None])
    weighted_queries = lax.dot_general(coefficient.astype(jnp.bfloat16), queries, (((0,), (0,)), ((), ())), preferred_element_type=jnp.float32)
    norm_term = lax.optimization_barrier(jnp.sum(coefficient * raw_score, axis=0))
    vec_change = passage_scale[:, None] * weighted_queries - vec_float * (passage_scale ** 3 * norm_term)[:, None]
    token_grad = (vec_change / divisor[:, None]).astype(jnp.bfloat16)
    block_grad = jnp.repeat(token_grad, 4, axis=0)[chosen].reshape(N_DP, CAP, D)

    def grad_group(triple):
        rows, mask, grad = triple
        row_float, rms_scale, gate, up, sigmoid_gate, branch = layer_forward(rows, norm_gain, w_gate, w_up, w_down)
        out_float = (mask[:, :, None] * grad[:, None, :].astype(jnp.float32)).reshape(CAP * block_len, D)
        out_grad = out_float.astype(jnp.bfloat16)
        hidden_grad = lax.dot_general(out_grad, w_down, (((1,), (1,)), ((), ())), preferred_element_type=jnp.float32)
        gate_grad = (hidden_grad * up * sigmoid_gate * (1.0 + gate * (1.0 - sigmoid_gate))).astype(jnp.bfloat16)
        up_grad = (hidden_grad * gate * sigmoid_gate).astype(jnp.bfloat16)
        normed_grad = lax.dot_general(gate_grad, w_gate, (((1,), (1,)), ((), ())), preferred_element_type=jnp.float32)
        normed_grad = normed_grad + lax.dot_general(up_grad, w_up, (((1,), (1,)), ((), ())), preferred_element_type=jnp.float32)
        inner = lax.optimization_barrier(jnp.mean(row_float * norm_gain[None, :] * normed_grad, axis=1))
        input_grad = out_float + rms_scale * norm_gain[None, :] * normed_grad - row_float * rms_scale ** 3 * inner[:, None]
        return input_grad.astype(jnp.bfloat16).reshape(CAP, block_len * D)
    task_grads = lax.map(grad_group, (task_rows, task_row_mask, block_grad)).reshape(N_DP * CAP, block_len * D)
    grad_rows = jnp.zeros((block_total, block_len * D), jnp.bfloat16).at[chosen].set(task_grads)
    return (query_loss, grad_rows.reshape(ROWS, D))
```

```python
import jax
import jax.numpy as jnp
from jax import lax
from jax.sharding import PartitionSpec as P

L = 128


pad_token = 128001
score_scale = 20.0
loss_seed = 4096.0
norm_epsilon = 1e-05
unit_epsilon = 1e-06
forward_chunks = 2
backward_chunks = 4
lane = 128


def contract_rows(left, right):
    return lax.dot_general(
        left, right, (((1,), (1,)), ((), ())), preferred_element_type=jnp.float32
    )


def exchange(value, bit, count):
    return lax.ppermute(value, "mp", [(i, i ^ bit) for i in range(count)])


def per_device(
    hidden_in, token_ids, passage_counts, positive_doc, queries, norm_gain, w_gate, w_up, w_down
):
    dp_count = lax.axis_size("dp")
    mp_count = lax.axis_size("mp")
    mp_index = lax.axis_index("mp")
    row_count, part_width = hidden_in.shape
    model_width = norm_gain.shape[0]
    docs_here = passage_counts.shape[0]
    passes_here = row_count // L
    most_pass = passes_here // docs_here
    query_count = queries.shape[0]
    halving = mp_count > 1 and mp_count & (mp_count - 1) == 0

    live_pass = jnp.arange(passes_here, dtype=jnp.int32) % most_pass < jnp.repeat(
        passage_counts, most_pass
    )
    token_live = (token_ids.reshape(passes_here, L) != pad_token) & live_pass[:, None]
    mask = token_live.astype(jnp.float32)
    divisor = jnp.maximum(jnp.sum(mask, axis=1), 1.0)

    chunk_rows = row_count // forward_chunks
    chunk_pass = passes_here // forward_chunks
    gathered = []
    for index in range(forward_chunks):
        piece = hidden_in[index * chunk_rows : (index + 1) * chunk_rows]
        if index == forward_chunks - 1:
            piece = jnp.concatenate([piece, queries], axis=0)
        gathered.append(lax.all_gather(piece, "mp", axis=1, tiled=True))
    full_queries = gathered[-1][chunk_rows:]

    gates, ups, scales, act_pools, row_pools = [], [], [], [], []
    for index in range(forward_chunks):
        row_float = gathered[index][:chunk_rows].astype(jnp.float32)
        rms_scale = lax.rsqrt(jnp.mean(row_float * row_float, axis=1, keepdims=True) + norm_epsilon)
        normed = (row_float * rms_scale * norm_gain[None, :]).astype(jnp.bfloat16)
        gate = jnp.dot(normed, w_gate, preferred_element_type=jnp.float32)
        up = jnp.dot(normed, w_up, preferred_element_type=jnp.float32)
        act = (gate * jax.nn.sigmoid(gate) * up).astype(jnp.bfloat16)
        weight = mask[index * chunk_pass : (index + 1) * chunk_pass, :, None]
        act_pools.append(
            jnp.sum(act.astype(jnp.float32).reshape(chunk_pass, L, -1) * weight, axis=1)
        )
        row_pools.append(jnp.sum(row_float.reshape(chunk_pass, L, model_width) * weight, axis=1))
        gates.append(gate)
        ups.append(up)
        scales.append(rms_scale)

    act_pool = jnp.concatenate(act_pools, axis=0)
    high = lax.reduce_precision(act_pool, 8, 7)
    both = jnp.concatenate([high, act_pool - high], axis=0).astype(jnp.bfloat16)
    branch = jnp.dot(both, w_down, preferred_element_type=jnp.float32)
    branch = (branch[:passes_here] + branch[passes_here:]).astype(jnp.bfloat16)
    branch_sum = jnp.sum(lax.all_gather(branch, "mp", axis=0).astype(jnp.float32), axis=0)
    passage_sum = jnp.concatenate(row_pools, axis=0) + branch_sum
    passage_vec = (passage_sum / divisor[:, None]).astype(jnp.bfloat16)

    flags = jnp.broadcast_to(live_pass[:, None], (passes_here, lane)).astype(jnp.bfloat16)
    payload = jnp.concatenate([passage_vec, flags], axis=1)
    everyone = lax.all_to_all(
        jnp.broadcast_to(payload[None], (dp_count,) + payload.shape),
        "dp",
        split_axis=0,
        concat_axis=0,
        tiled=True,
    ).reshape(dp_count * passes_here, model_width + lane)
    all_vec = everyone[:, :model_width]
    all_live = everyone[:, model_width].astype(jnp.float32)
    pass_total = dp_count * passes_here
    doc_total = dp_count * docs_here

    vec_float = all_vec.astype(jnp.float32)
    query_float = full_queries.astype(jnp.float32)
    raw_score = contract_rows(full_queries, all_vec)
    query_scale = lax.rsqrt(jnp.sum(query_float * query_float, axis=1) + unit_epsilon)
    passage_scale = lax.rsqrt(jnp.sum(vec_float * vec_float, axis=1) + unit_epsilon)
    scores = score_scale * raw_score * query_scale[:, None] * passage_scale[None, :]
    weights = all_live[None, :] * jnp.exp(scores)
    positive_pass = (
        positive_doc[:, None] == (jnp.arange(pass_total, dtype=jnp.int32) // most_pass)[None, :]
    ).astype(jnp.float32)
    total_mass = jnp.sum(weights, axis=1)
    positive_mass = jnp.sum(weights * positive_pass, axis=1)
    query_loss = jnp.log(total_mass) - jnp.log(positive_mass)
    coefficient = (
        loss_seed
        * score_scale
        * query_scale[:, None]
        * (weights / total_mass[:, None] - positive_pass * weights / positive_mass[:, None])
    )
    weighted_queries = lax.dot_general(
        coefficient.astype(jnp.bfloat16),
        full_queries,
        (((0,), (0,)), ((), ())),
        preferred_element_type=jnp.float32,
    )
    norm_term = jnp.sum(coefficient * raw_score, axis=0)
    terms = jnp.concatenate(
        [weighted_queries, jnp.broadcast_to(norm_term[:, None], (pass_total, lane))], axis=1
    ).astype(jnp.bfloat16)
    terms = lax.all_to_all(
        terms.reshape(dp_count, passes_here, model_width + lane),
        "dp",
        split_axis=0,
        concat_axis=0,
        tiled=True,
    )
    terms = jnp.sum(terms.astype(jnp.float32), axis=0)
    own_vec = passage_vec.astype(jnp.float32)
    own_scale = lax.rsqrt(jnp.sum(own_vec * own_vec, axis=1) + unit_epsilon)
    vec_change = (
        own_scale[:, None] * terms[:, :model_width]
        - own_vec * (own_scale**3 * terms[:, model_width])[:, None]
    )
    token_grad = (vec_change / divisor[:, None]).astype(jnp.bfloat16)
    own_token_grad = lax.dynamic_slice_in_dim(
        token_grad, mp_index * part_width, part_width, 1
    ).astype(jnp.float32)
    own_gain = lax.dynamic_slice_in_dim(norm_gain, mp_index * part_width, part_width)

    pass_grad = contract_rows(token_grad, w_down)

    def weight_rows(distance):
        start = (mp_index ^ distance) * part_width
        return jnp.concatenate(
            [
                lax.dynamic_slice_in_dim(w_gate, start, part_width, 0),
                lax.dynamic_slice_in_dim(w_up, start, part_width, 0),
            ],
            axis=1,
        )

    if halving:
        far = [j for j in range(mp_count) if j & 1]
        near = [j ^ 1 for j in far]
        far_rows = jnp.concatenate([weight_rows(j) for j in far], axis=0)
        near_rows = jnp.concatenate([weight_rows(j) for j in near], axis=0)
        far_rows, near_rows = lax.optimization_barrier((far_rows, near_rows))

    back_pass = passes_here // backward_chunks
    back_rows = row_count // backward_chunks
    per_forward = backward_chunks // forward_chunks
    grads, inner_parts = [], []
    for index in range(backward_chunks):
        low = (index % per_forward) * back_rows
        gate = gates[index // per_forward][low : low + back_rows]
        up = ups[index // per_forward][low : low + back_rows]
        own_pass = slice(index * back_pass, (index + 1) * back_pass)
        weight = mask[own_pass, :, None]
        dact = (weight * pass_grad[own_pass, None, :]).reshape(back_rows, -1)
        sigmoid_gate = jax.nn.sigmoid(gate)
        gate_grad = (dact * up * sigmoid_gate * (1.0 + gate * (1.0 - sigmoid_gate))).astype(
            jnp.bfloat16
        )
        up_grad = (dact * gate * sigmoid_gate).astype(jnp.bfloat16)
        inner_parts.append(
            jnp.sum(gate_grad.astype(jnp.float32) * gate + up_grad.astype(jnp.float32) * up, axis=1)
        )
        if halving:
            both_grads = lax.optimization_barrier(jnp.concatenate([gate_grad, up_grad], axis=1))
            sent = contract_rows(both_grads, far_rows).astype(jnp.bfloat16)
            kept = contract_rows(both_grads, near_rows)
            kept = kept + exchange(sent, 1, mp_count).astype(jnp.float32)
            bit = 2
            while bit < mp_count:
                blocks = [
                    kept[:, i * part_width : (i + 1) * part_width]
                    for i in range(kept.shape[1] // part_width)
                ]
                sent = jnp.concatenate(blocks[1::2], axis=1).astype(jnp.bfloat16)
                kept = jnp.concatenate(blocks[0::2], axis=1)
                kept = kept + exchange(sent, bit, mp_count).astype(jnp.float32)
                bit *= 2
        else:
            normed_grad = contract_rows(gate_grad, w_gate) + contract_rows(up_grad, w_up)
            kept = lax.psum_scatter(
                normed_grad.astype(jnp.bfloat16), "mp", scatter_dimension=1, tiled=True
            ).astype(jnp.float32)
        grads.append(kept)

    inner = jnp.sum(lax.all_gather(jnp.concatenate(inner_parts)[None, :], "mp", axis=0), axis=0)[0]
    results = []
    for index in range(backward_chunks):
        own_pass = slice(index * back_pass, (index + 1) * back_pass)
        rows = slice(index * back_rows, (index + 1) * back_rows)
        low = (index % per_forward) * back_rows
        rms_scale = scales[index // per_forward][low : low + back_rows]
        own_out = (mask[own_pass, :, None] * own_token_grad[own_pass, None, :]).reshape(
            back_rows, part_width
        )
        own_input = hidden_in[rows].astype(jnp.float32)
        results.append(
            (
                own_out
                + rms_scale * own_gain[None, :] * grads[index]
                - own_input * rms_scale**2 * (inner[rows, None] / model_width)
            ).astype(jnp.bfloat16)
        )
    return (query_loss, jnp.concatenate(results, axis=0))


def solution(mesh):
    return jax.shard_map(
        per_device,
        mesh=mesh,
        in_specs=(
            P("dp", "mp"),
            P("dp"),
            P("dp"),
            P("dp"),
            P("dp", "mp"),
            P(),
            P(None, "mp"),
            P(None, "mp"),
            P("mp", None),
        ),
        out_specs=(P("dp"), P("dp", "mp")),
        check_vma=False,
    )
```
